8 devices in a mesh: pod: 2 (over z, y), data: 4 (over x, core).
Axes of the slice: x: 2, y: 2, z: 1, core: 2. Of those that a mesh axis runs over, the one named last changes fastest.
Arguments:
- feat_a: bfloat16 [8192, 2048], P(('pod', 'data'))
- feat_b: bfloat16 [8192, 2048], P(('pod', 'data'))
- w_first: bfloat16 [2048, 4096], replicated
- w_second: bfloat16 [4096, 4096], replicated
- w_third: bfloat16 [4096, 4096], replicated
- gain_first: float32 [4096], replicated
- shift_first: float32 [4096], replicated
- gain_second: float32 [4096], replicated
- shift_second: float32 [4096], replicated
- lam_off: float32 [], replicated
Outputs:
- output 1: float32 [], replicated
- output 2: float32 [2048, 4096], replicated
- output 3: float32 [4096, 4096], replicated
- output 4: float32 [4096, 4096], replicated
- output 5: float32 [4096], replicated
- output 6: float32 [4096], replicated
- output 7: float32 [4096], replicated
- output 8: float32 [4096], replicated
All inputs are finite; a program needn't handle non-finite values.
Results may differ from the reference program's by a relative error of at most 0.00104.
Values are sent between devices in bfloat16 or wider.
A program may use at most 1 GiB of HBM per device.

```python
import jax
import jax.numpy as jnp
from jax import lax

ROWS_DEV = 1024
NUM_DEVICES = 8
FEAT_DIM = 2048
PROJ_DIM = 4096
NUM_ROWS = ROWS_DEV * NUM_DEVICES
BN_EPS = 1e-5


def setup_inputs(seed: int = 0) -> dict:
    key_list = jax.random.split(jax.random.key(seed), 12)
    block_shape = (NUM_DEVICES, ROWS_DEV, FEAT_DIM)
    stat_shape = (NUM_DEVICES, 1, FEAT_DIM)
    base_vals = jax.random.normal(key_list[0], block_shape, jnp.float32)
    noise_vals = jax.random.normal(key_list[1], block_shape, jnp.float32)
    shard_shift = 0.7 * jax.random.normal(key_list[2], stat_shape, jnp.float32)
    shard_scale = jax.random.uniform(key_list[3], stat_shape, jnp.float32, 0.5, 1.5)
    view_a = base_vals * shard_scale + shard_shift
    view_b = (0.8 * base_vals + 0.6 * noise_vals) * shard_scale + shard_shift
    w_first = jax.random.normal(key_list[4], (FEAT_DIM, PROJ_DIM), jnp.float32) * FEAT_DIM ** -0.5
    w_second = jax.random.normal(key_list[5], (PROJ_DIM, PROJ_DIM), jnp.float32) * PROJ_DIM ** -0.5
    w_third = jax.random.normal(key_list[6], (PROJ_DIM, PROJ_DIM), jnp.float32) * PROJ_DIM ** -0.5
    lam_off = (0.05 + 0.1 * jax.random.uniform(key_list[11], (), jnp.float32)) * NUM_ROWS / PROJ_DIM
    return {
        'feat_a': view_a.reshape(NUM_ROWS, FEAT_DIM).astype(jnp.bfloat16),
        'feat_b': view_b.reshape(NUM_ROWS, FEAT_DIM).astype(jnp.bfloat16),
        'w_first': w_first.astype(jnp.bfloat16),
        'w_second': w_second.astype(jnp.bfloat16),
        'w_third': w_third.astype(jnp.bfloat16),
        'gain_first': 1.0 + 0.3 * jax.random.normal(key_list[7], (PROJ_DIM,), jnp.float32),
        'shift_first': 0.5 * jax.random.normal(key_list[8], (PROJ_DIM,), jnp.float32),
        'gain_second': 1.0 + 0.3 * jax.random.normal(key_list[9], (PROJ_DIM,), jnp.float32),
        'shift_second': 0.5 * jax.random.normal(key_list[10], (PROJ_DIM,), jnp.float32),
        'lam_off': lam_off,
    }


def batch_norm(pre_act):
    feat_mean = jnp.sum(pre_act, axis=0) / NUM_ROWS
    sq_mean = jnp.sum(pre_act * pre_act, axis=0) / NUM_ROWS
    inv_std = lax.rsqrt(sq_mean - feat_mean * feat_mean + BN_EPS)
    return (pre_act - feat_mean) * inv_std, inv_std


def project(feats_in, w_first, w_second, w_third, gain_first, shift_first, gain_second, shift_second):
    pre_one = jnp.dot(feats_in, w_first, preferred_element_type=jnp.float32)
    norm_one, inv_one = batch_norm(pre_one)
    post_one = gain_first * norm_one + shift_first
    hid_one = jnp.maximum(post_one, 0.0).astype(jnp.bfloat16)
    pre_two = jnp.dot(hid_one, w_second, preferred_element_type=jnp.float32)
    norm_two, inv_two = batch_norm(pre_two)
    post_two = gain_second * norm_two + shift_second
    hid_two = jnp.maximum(post_two, 0.0).astype(jnp.bfloat16)
    proj_out = jnp.dot(hid_two, w_third, preferred_element_type=jnp.float32)
    emb_norm, inv_three = batch_norm(proj_out)
    return (norm_one, inv_one, post_one, hid_one, norm_two, inv_two, post_two, hid_two, emb_norm, inv_three)


def norm_backward(grad_norm, normed, inv_std):
    grad_mean = jnp.sum(grad_norm, axis=0) / NUM_ROWS
    cross_mean = jnp.sum(grad_norm * normed, axis=0) / NUM_ROWS
    return inv_std * (grad_norm - grad_mean - normed * cross_mean)


def back_project(grad_emb, feats_in, saved, w_second, w_third, gain_first, gain_second):
    norm_one, inv_one, post_one, hid_one, norm_two, inv_two, post_two, hid_two, emb_norm, inv_three = saved
    grad_proj = norm_backward(grad_emb, emb_norm, inv_three).astype(jnp.bfloat16)
    grad_third = jnp.dot(hid_two.T, grad_proj, preferred_element_type=jnp.float32)
    grad_act_two = jnp.where(post_two > 0, jnp.dot(grad_proj, w_third.T, preferred_element_type=jnp.float32), 0.0)
    grad_gain_two = jnp.sum(grad_act_two * norm_two, axis=0)
    grad_shift_two = jnp.sum(grad_act_two, axis=0)
    grad_pre_two = norm_backward(gain_second * grad_act_two, norm_two, inv_two).astype(jnp.bfloat16)
    grad_second = jnp.dot(hid_one.T, grad_pre_two, preferred_element_type=jnp.float32)
    grad_act_one = jnp.where(post_one > 0, jnp.dot(grad_pre_two, w_second.T, preferred_element_type=jnp.float32), 0.0)
    grad_gain_one = jnp.sum(grad_act_one * norm_one, axis=0)
    grad_shift_one = jnp.sum(grad_act_one, axis=0)
    grad_pre_one = norm_backward(gain_first * grad_act_one, norm_one, inv_one).astype(jnp.bfloat16)
    grad_first = jnp.dot(feats_in.T, grad_pre_one, preferred_element_type=jnp.float32)
    return (grad_first, grad_second, grad_third, grad_gain_one, grad_shift_one, grad_gain_two, grad_shift_two)


def reference(feat_a, feat_b, w_first, w_second, w_third, gain_first, shift_first, gain_second, shift_second, lam_off):
    saved_a = project(feat_a, w_first, w_second, w_third, gain_first, shift_first, gain_second, shift_second)
    saved_b = project(feat_b, w_first, w_second, w_third, gain_first, shift_first, gain_second, shift_second)
    emb_a = saved_a[8].astype(jnp.bfloat16)
    emb_b = saved_b[8].astype(jnp.bfloat16)
    corr_mat = jnp.dot(emb_a.T, emb_b, preferred_element_type=jnp.float32) / NUM_ROWS
    on_diag = jnp.diagonal(corr_mat)
    total_loss = jnp.sum((1.0 - on_diag) ** 2) + lam_off * (jnp.sum(corr_mat * corr_mat) - jnp.sum(on_diag * on_diag))
    diag_mask = jnp.arange(PROJ_DIM)[:, None] == jnp.arange(PROJ_DIM)[None, :]
    grad_corr = jnp.where(diag_mask, -2.0 * (1.0 - corr_mat), 2.0 * lam_off * corr_mat).astype(jnp.bfloat16)
    grad_emb_a = jnp.dot(emb_b, grad_corr.T, preferred_element_type=jnp.float32) / NUM_ROWS
    grad_emb_b = jnp.dot(emb_a, grad_corr, preferred_element_type=jnp.float32) / NUM_ROWS
    grads_a = back_project(grad_emb_a, feat_a, saved_a, w_second, w_third, gain_first, gain_second)
    grads_b = back_project(grad_emb_b, feat_b, saved_b, w_second, w_third, gain_first, gain_second)
    return (total_loss, grads_a[0] + grads_b[0], grads_a[1] + grads_b[1], grads_a[2] + grads_b[2], grads_a[3] + grads_b[3], grads_a[4] + grads_b[4], grads_a[5] + grads_b[5], grads_a[6] + grads_b[6])
```

```python
import functools
import jax
import jax.numpy as jnp
from jax import lax
from jax.sharding import PartitionSpec as P

BN_EPS = 1e-5
ROW_AXES = ('pod', 'data')
F32 = jnp.float32
BF16 = jnp.bfloat16
CORE, XDIM, YDIM = 1, 2, 4


def swap(value, bit):
    return lax.ppermute(value, ROW_AXES, [(i, i ^ bit) for i in range(8)])


def my_bits():
    data = lax.axis_index('data')
    return {CORE: data % 2, XDIM: data // 2, YDIM: lax.axis_index('pod')}


def sum_small(value):
    for bit in (CORE, XDIM, YDIM):
        value = value + swap(value, bit)
    return value


def dot_t(lhs, rhs):
    return lax.dot_general(lhs, rhs, (((0,), (0,)), ((), ())), preferred_element_type=F32)


def rows_at(value, start, size):
    return lax.dynamic_slice(value, (start, 0), (size, value.shape[1]))


def cols_at(value, start, size):
    return lax.dynamic_slice(value, (0, start), (value.shape[0], size))


def reduce_block(lhs, rhs, base, rows, order, bits):
    half = rows // 2
    core = bits[CORE]
    sent = swap(dot_t(cols_at(lhs, base + (1 - core) * half, half), rhs), CORE)
    value = dot_t(cols_at(lhs, base + core * half, half), rhs) + sent
    size = half
    for bit in order:
        size //= 2
        mine = bits[bit]
        recv = swap(rows_at(value, (1 - mine) * size, size), bit)
        value = rows_at(value, mine * size, size) + recv
    start = base + core * half + bits[order[0]] * (half // 2) + bits[order[1]] * (half // 4)
    return value, start


def gather_block(out, piece, base, rows, order, bits):
    size = rows // 8
    first, second = order

    def place(buf, val, core, one, two):
        return lax.dynamic_update_slice(buf, val, (base + (core * 4 + one * 2 + two) * size, 0))

    core, one, two = bits[CORE], bits[first], bits[second]
    held = [(piece, one, two)]
    out = place(out, piece, core, one, two)
    other = swap(piece, second)
    held.append((other, one, 1 - two))
    out = place(out, other, core, one, 1 - two)
    for val, _, tw in list(held):
        other = swap(val, first)
        held.append((other, 1 - one, tw))
        out = place(out, other, core, 1 - one, tw)
    for val, on, tw in held:
        out = place(out, swap(val, CORE), 1 - core, on, tw)
    return out


def blocks_of(rows, count):
    size = rows // count
    return [(k * size, size, (XDIM, YDIM) if k % 2 == 0 else (YDIM, XDIM)) for k in range(count)]


def sum_grad(lhs, rhs, count, bits):
    rows = lhs.shape[1]
    out = jnp.zeros((rows, rhs.shape[1]), F32)
    pieces = [(reduce_block(lhs, rhs, base, size, order, bits), base, size, order) for base, size, order in blocks_of(rows, count)]
    for (piece, _), base, size, order in pieces:
        out = gather_block(out, piece, base, size, order, bits)
    return out


def batch_norm(pre_act, num_rows):
    totals = sum_small(jnp.stack([jnp.sum(pre_act, axis=1), jnp.sum(pre_act * pre_act, axis=1)])) / num_rows
    inv_std = lax.rsqrt(totals[1] - totals[0] * totals[0] + BN_EPS)[:, None, :]
    return (pre_act - totals[0][:, None, :]) * inv_std, inv_std


def run_layer(hidden, weight, gain_vec, shift_vec, num_rows):
    pre_act = jnp.einsum('vnf,fd->vnd', hidden, weight, preferred_element_type=F32)
    normed, inv_std = batch_norm(pre_act, num_rows)
    post_affine = gain_vec * normed + shift_vec
    return jnp.maximum(post_affine, 0.0).astype(BF16), post_affine, normed, inv_std


def norm_backward(grad_norm, normed, inv_std, num_rows):
    totals = sum_small(jnp.stack([jnp.sum(grad_norm, axis=1), jnp.sum(grad_norm * normed, axis=1)])) / num_rows
    return inv_std * (grad_norm - totals[0][:, None, :] - normed * totals[1][:, None, :])


def affine_backward(grad_hid, post_affine, normed, inv_std, gain_vec, num_rows):
    grad_act = jnp.where(post_affine > 0, grad_hid, 0.0)
    totals = sum_small(jnp.stack([jnp.sum(grad_act * normed, axis=1), jnp.sum(grad_act, axis=1)]))
    grad_pre = (gain_vec * inv_std) * (grad_act - totals[1][:, None, :] / num_rows - normed * (totals[0][:, None, :] / num_rows))
    return grad_pre.astype(BF16), jnp.sum(totals[0], axis=0), jnp.sum(totals[1], axis=0)


def device_step(num_dev, feat_a, feat_b, w_first, w_second, w_third, gain_first, shift_first, gain_second, shift_second, lam_off):
    num_rows = feat_a.shape[0] * num_dev
    bits = my_bits()
    both_views = jnp.stack([feat_a, feat_b])
    hid_one, post_one, norm_one, inv_one = run_layer(both_views, w_first, gain_first, shift_first, num_rows)
    hid_two, post_two, norm_two, inv_two = run_layer(hid_one, w_second, gain_second, shift_second, num_rows)
    proj_out = jnp.einsum('vnf,fd->vnd', hid_two, w_third, preferred_element_type=F32)
    emb_norm, inv_three = batch_norm(proj_out, num_rows)
    emb_bf = emb_norm.astype(BF16)

    dim = emb_bf.shape[2]
    pieces = []
    loss = jnp.zeros((), F32)
    for base, size, order in blocks_of(dim, 4):
        corr, start = reduce_block(emb_bf[0], emb_bf[1], base, size, order, bits)
        corr = corr / num_rows
        diag = (lax.broadcasted_iota(jnp.int32, corr.shape, 0) + start) == lax.broadcasted_iota(jnp.int32, corr.shape, 1)
        pieces.append((jnp.where(diag, -2.0 * (1.0 - corr), 2.0 * lam_off * corr).astype(BF16), base, size, order))
        loss = loss + jnp.sum(jnp.where(diag, (1.0 - corr) * (1.0 - corr), lam_off * (corr * corr)))
    total_loss = sum_small(jnp.full((8, 128), loss, F32))[0, 0]
    grad_a, grad_b = [], None
    for piece, base, size, order in pieces:
        block = gather_block(jnp.zeros((size, dim), BF16), piece, 0, size, order, bits)
        grad_a.append(lax.dot_general(emb_bf[1], block, (((1,), (1,)), ((), ())), preferred_element_type=F32))
        part = jnp.dot(emb_bf[0, :, base:base + size], block, preferred_element_type=F32)
        grad_b = part if grad_b is None else grad_b + part
    grad_emb = jnp.stack([jnp.concatenate(grad_a, axis=1), grad_b]) / num_rows

    def flat(value):
        return value.reshape(-1, value.shape[-1])

    grad_proj = norm_backward(grad_emb, emb_norm, inv_three, num_rows).astype(BF16)
    grad_third = sum_grad(flat(hid_two), flat(grad_proj), 4, bits)
    grad_hid_two = jnp.einsum('wof,ef->woe', grad_proj, w_third, preferred_element_type=F32)
    grad_pre_two, grad_gain_second, grad_shift_second = affine_backward(grad_hid_two, post_two, norm_two, inv_two, gain_second, num_rows)
    grad_second = sum_grad(flat(hid_one), flat(grad_pre_two), 4, bits)
    grad_hid_one = jnp.einsum('wof,ef->woe', grad_pre_two, w_second, preferred_element_type=F32)
    grad_pre_one, grad_gain_first, grad_shift_first = affine_backward(grad_hid_one, post_one, norm_one, inv_one, gain_first, num_rows)
    grad_first = sum_grad(flat(both_views), flat(grad_pre_one), 4, bits)
    return (total_loss, grad_first, grad_second, grad_third, grad_gain_first, grad_shift_first, grad_gain_second, grad_shift_second)


def solution(mesh):
    num_dev = mesh.shape['pod'] * mesh.shape['data']
    row_spec = P(ROW_AXES, None)
    repl_spec = P()
    return jax.shard_map(functools.partial(device_step, num_dev), mesh=mesh, in_specs=(row_spec, row_spec) + (repl_spec,) * 8, out_specs=(repl_spec,) * 8, check_vma=False)
```
